32 devices in a mesh: circ: 8 (over z, y), side: 4 (over x, core).
Axes of the slice: x: 2, y: 2, z: 4, core: 2. Of those that a mesh axis runs over, the one named last changes fastest.
Arguments:
- field: float32 [4, 7, 7, 7, 8, 1024], P('side', None, None, None, None, 'circ'), may hold values from -6 to 6
- coeffs: float32 [4, 3, 7, 7, 7, 8, 1024], P('side', None, None, None, None, None, 'circ'), may hold values from 0.25 to 1.5
- reaction: float32 [4, 7, 7, 7, 8, 1024], P('side', None, None, None, None, 'circ'), may hold values from 0.25 to 8
- step_scale: float32 [4, 7, 7, 7, 8, 1024], P('side', None, None, None, None, 'circ'), may hold values from 0.0001 to 0.0003
- rotation: int32 [4], replicated, may hold values from 0 to 3071
Outputs:
- advanced: float32 [4, 7, 7, 7, 8, 1024], P('side', None, None, None, None, 'circ')
The draws below stay inside these ranges and needn't reach their ends.
Inputs may be any that keep to these rules, and one draw needn't show every extreme that they name: `rotation`: rotor position in units of one 3-th of an element's circumferential width.
All inputs are finite; a program needn't handle non-finite values.
Results may differ from the reference program's by a relative error of at most 0.0001.
Values sent between devices are 32-bit elements; how exact they have to be, the bound alone decides.
A program may use at most 128 MiB of HBM per device.

```python
import math
import jax
import jax.numpy as jnp
import numpy as np
from jax import lax

NODES = 7
ER = 8
SUBSTEPS = 3
STEPS = 4
LAYERS = 4
NC = 1024


def plant(drawn, rng, smallest, top_value):
    dims = drawn.shape
    place = [jax.random.randint(jax.random.fold_in(rng, axis), (), 0, dims[axis]) for axis in range(len(dims))]
    drawn = drawn.at[tuple(place)].set(smallest)
    longest = dims.index(max(dims))
    place[longest] = (place[longest] + 1) % dims[longest]
    return drawn.at[tuple(place)].set(top_value)


def level_of(own_key, dims, shards, least, top_value):
    level, own = 1.0, jax.random.fold_in(own_key, 6)
    for axis_at, shards_of in shards:
        steps = jnp.exp(jax.random.uniform(jax.random.fold_in(own, axis_at), (shards_of,), jnp.float32, least / len(shards), top_value / len(shards)))
        level = level * jnp.repeat(steps, dims[axis_at] // shards_of).reshape([-1 if axis == axis_at else 1 for axis in range(len(dims))])
    return level


def noise(own_key, extent, scale, limit, pieces=(), held_as=jnp.bfloat16):
    entries = jax.random.normal(own_key, extent, jnp.float32) * scale
    if len(pieces) > 0:
        entries = level_of(own_key, extent, pieces, -0.22, 0.18) * entries
    return jnp.clip(entries, min=-limit, max=limit).astype(held_as)


def setup_inputs(seed: int = 0) -> dict:
    keys = jax.random.split(jax.random.key(seed), 6)
    field = noise(keys[0], (LAYERS, NODES, NODES, NODES, ER, NC), 1.0, 6.0, ((0, 4), (5, 8)), jnp.float32)
    coeffs = jnp.clip(jnp.exp(math.log(1.5) - 1.7917595 * jax.random.uniform(keys[1], (LAYERS, 3, NODES, NODES, NODES, ER, NC), jnp.float32) ** level_of(keys[1], (LAYERS, 3, NODES, NODES, NODES, ER, NC), ((0, 4), (6, 8)), -0.2, 0.2)), 0.25, 1.5)
    reaction = jnp.clip(jnp.exp(math.log(8.0) - 3.465736 * jax.random.uniform(keys[2], (LAYERS, NODES, NODES, NODES, ER, NC), jnp.float32) ** level_of(keys[2], (LAYERS, NODES, NODES, NODES, ER, NC), ((0, 4), (5, 8)), -0.2, 0.2)), 0.25, 8.0)
    step_scale = jnp.clip(jnp.exp(math.log(0.0003) - 1.09861236 * jax.random.uniform(keys[3], (LAYERS, NODES, NODES, NODES, ER, NC), jnp.float32) ** level_of(keys[3], (LAYERS, NODES, NODES, NODES, ER, NC), ((0, 4), (5, 8)), -0.2, 0.2)), 0.0001, 0.0003)
    rotation = plant(jax.random.randint(keys[4], (STEPS,), 0, NC * SUBSTEPS), jax.random.fold_in(keys[4], 1), 0, (NC * SUBSTEPS) - 1).astype(jnp.int32)
    return {"field": field, "coeffs": coeffs, "reaction": reaction, "step_scale": step_scale, "rotation": rotation}


def gll_points():
    return np.array([-1.0, -0.830223896278567, -0.4688487934707142, 0.0, 0.4688487934707142, 0.830223896278567, 1.0])


def derivative_table():
    points = gll_points()
    node_count = points.shape[0]
    weights = np.array([1.0 / np.prod([points[j] - points[k] for k in range(node_count) if k != j]) for j in range(node_count)])
    derivative = np.zeros((node_count, node_count))
    for i in range(node_count):
        for j in range(node_count):
            if i != j:
                derivative[i, j] = weights[j] / weights[i] / (points[i] - points[j])
        derivative[i, i] = -np.sum(derivative[i])
    return derivative


def lagrange_rows(locations):
    points = gll_points()
    identity_mask = np.eye(7) > 0.5
    differences = np.array([[1.0 if q == n else points[n] - points[q] for q in range(7)] for n in range(7)])
    denominator = np.prod(differences, axis=1)
    distances = locations[:, None] - jnp.asarray(points, jnp.float32)[None, :]
    factors = jnp.where(identity_mask[None, :, :], 1.0, distances[:, None, :])
    return jnp.prod(factors, axis=2) / jnp.asarray(denominator, jnp.float32)[None, :]


def mortar_tables(fraction):
    heights = (1.0 + jnp.asarray(gll_points(), jnp.float32)) * 0.5
    on_right = heights >= fraction
    shifted_height = jnp.where(on_right, heights - fraction, heights - fraction + 1.0)
    values = lagrange_rows(2.0 * shifted_height - 1.0)
    from_right = jnp.where(on_right[:, None], values, 0.0)
    from_left = jnp.where(on_right[:, None], 0.0, values)
    return from_left, from_right


def element_apply(field, coeffs, reaction):
    derivative = jnp.asarray(derivative_table(), jnp.float32)
    highest = lax.Precision.HIGHEST
    grad_axial = jnp.einsum("pa,arcxe->prcxe", derivative, field, precision=highest)
    grad_radial = jnp.einsum("pr,arcxe->apcxe", derivative, field, precision=highest)
    grad_circ = jnp.einsum("pc,arcxe->arpxe", derivative, field, precision=highest)
    result = reaction * field
    result = result + jnp.einsum("pa,prcxe->arcxe", derivative, coeffs[0] * grad_axial, precision=highest)
    result = result + jnp.einsum("pr,apcxe->arcxe", derivative, coeffs[1] * grad_radial, precision=highest)
    result = result + jnp.einsum("pc,arpxe->arcxe", derivative, coeffs[2] * grad_circ, precision=highest)
    return result


def layer_apply(inputs):
    return element_apply(inputs[0], inputs[1], inputs[2])


def reference(field, coeffs, reaction, step_scale, rotation):
    lower = LAYERS // 2 - 1
    highest = lax.Precision.HIGHEST
    current = field
    for step in range(STEPS):
        applied = lax.map(layer_apply, (current, coeffs, reaction))
        outer_faces = applied[:, :, 6]
        inner_faces = applied[:, :, 0]
        zero_row = jnp.zeros_like(inner_faces[:, :, :, :1])
        summed = applied.at[:, :, 6].add(jnp.concatenate([inner_faces[:, :, :, 1:], zero_row], axis=3))
        summed = summed.at[:, :, 0].add(jnp.concatenate([zero_row, outer_faces[:, :, :, :-1]], axis=3))
        summed = summed.at[:, :, :, 6].add(jnp.roll(applied[:, :, :, 0], -1, axis=4))
        summed = summed.at[:, :, :, 0].add(jnp.roll(applied[:, :, :, 6], 1, axis=4))
        top_faces = applied[:, 6]
        bottom_faces = applied[:, 0]
        offset = rotation[step]
        whole_k = (offset // SUBSTEPS).astype(jnp.int32)
        fraction = (offset % SUBSTEPS).astype(jnp.float32) / SUBSTEPS
        from_left, from_right = mortar_tables(fraction)
        rotor_top = top_faces[lower]
        stator_bottom = bottom_faces[lower + 1]
        stator_part = jnp.einsum("mn,rnxe->rmxe", from_left, jnp.roll(rotor_top, whole_k + 1, axis=3), precision=highest)
        stator_part = stator_part + jnp.einsum("mn,rnxe->rmxe", from_right, jnp.roll(rotor_top, whole_k, axis=3), precision=highest)
        rotor_part = jnp.einsum("mn,rmxe->rnxe", from_right, jnp.roll(stator_bottom, -whole_k, axis=3), precision=highest)
        rotor_part = rotor_part + jnp.einsum("mn,rmxe->rnxe", from_left, jnp.roll(stator_bottom, -whole_k - 1, axis=3), precision=highest)
        zero_face = jnp.zeros_like(top_faces[:1])
        from_below = jnp.concatenate([zero_face, top_faces[:-1]], axis=0)
        from_above = jnp.concatenate([bottom_faces[1:], zero_face], axis=0)
        from_below = from_below.at[lower + 1].set(stator_part)
        from_above = from_above.at[lower].set(rotor_part)
        summed = summed.at[:, 0].add(from_below)
        summed = summed.at[:, 6].add(from_above)
        current = current - step_scale * summed
    return current
```

```python
from functools import partial

import jax
import jax.numpy as jnp
import numpy as np
from jax import lax
from jax.experimental import pallas as pl
from jax.experimental.pallas import tpu as pltpu
from jax.sharding import PartitionSpec as P

SUBSTEPS = 3
STEPS = 4


def passed_along(value, axis, steps):
    count = lax.axis_size(axis)
    pairs = [(source, (source + steps) % count) for source in range(count)]
    return lax.ppermute(value, axis, pairs)


def padded_2(block, sides, width, periodic):
    for axis, dim in sides:
        count = lax.axis_size(axis)
        forward = [(i, i + 1) for i in range(count - 1)]
        if periodic:
            forward.append((count - 1, 0))
        backward = [(target, source) for source, target in forward]
        low = lax.ppermute(
            lax.slice_in_dim(block, block.shape[dim] - width, None, axis=dim), axis, forward
        )
        high = lax.ppermute(lax.slice_in_dim(block, 0, width, axis=dim), axis, backward)
        block = jnp.concatenate([low, block, high], axis=dim)
    return block


def gll_points():
    return np.array(
        [
            -1.0,
            -0.830223896278567,
            -0.4688487934707142,
            0.0,
            0.4688487934707142,
            0.830223896278567,
            1.0,
        ]
    )


def derivative_table():
    points = gll_points()
    node_count = points.shape[0]
    weights = np.array(
        [
            1.0 / np.prod([points[j] - points[k] for k in range(node_count) if k != j])
            for j in range(node_count)
        ]
    )
    derivative = np.zeros((node_count, node_count))
    for i in range(node_count):
        for j in range(node_count):
            if i != j:
                derivative[i, j] = weights[j] / weights[i] / (points[i] - points[j])
        derivative[i, i] = -np.sum(derivative[i])
    return derivative


def lagrange_rows(locations):
    points = gll_points()
    identity_mask = np.eye(7) > 0.5
    differences = np.array(
        [[1.0 if q == n else points[n] - points[q] for q in range(7)] for n in range(7)]
    )
    denominator = np.prod(differences, axis=1)
    distances = locations[:, None] - jnp.asarray(points, jnp.float32)[None, :]
    factors = jnp.where(identity_mask[None, :, :], 1.0, distances[:, None, :])
    return jnp.prod(factors, axis=2) / jnp.asarray(denominator, jnp.float32)[None, :]


def mortar_tables(fraction):
    heights = (1.0 + jnp.asarray(gll_points(), jnp.float32)) * 0.5
    on_right = heights >= fraction
    shifted_height = jnp.where(on_right, heights - fraction, heights - fraction + 1.0)
    values = lagrange_rows(2.0 * shifted_height - 1.0)
    from_right = jnp.where(on_right[:, None], values, 0.0)
    from_left = jnp.where(on_right[:, None], 0.0, values)
    return (from_left, from_right)


def element_apply(field, coeffs, reaction):
    derivative = jnp.asarray(derivative_table(), jnp.float32)
    highest = lax.Precision.HIGHEST
    grad_axial = jnp.einsum("pa,arcxe->prcxe", derivative, field, precision=highest)
    grad_radial = jnp.einsum("pr,arcxe->apcxe", derivative, field, precision=highest)
    grad_circ = jnp.einsum("pc,arcxe->arpxe", derivative, field, precision=highest)
    result = reaction * field
    result = result + jnp.einsum(
        "pa,prcxe->arcxe", derivative, coeffs[0] * grad_axial, precision=highest
    )
    result = result + jnp.einsum(
        "pr,apcxe->arcxe", derivative, coeffs[1] * grad_radial, precision=highest
    )
    result = result + jnp.einsum(
        "pc,arpxe->arcxe", derivative, coeffs[2] * grad_circ, precision=highest
    )
    return result


def fixed_pair(hops, circ_count, is_stator, data):
    ahead = passed_along(data, "circ", hops)
    behind = passed_along(data, "circ", (circ_count - hops - 1) % circ_count)
    return jnp.where(is_stator, ahead, behind)


def rotate_window(block, amount, whole_k, is_stator):
    edge_count = block.shape[-1]
    circ_count = lax.axis_size("circ")
    within = amount % edge_count
    sector_k = whole_k // edge_count
    branches = [partial(fixed_pair, hops, circ_count, is_stator) for hops in range(circ_count)]
    rotated = lax.switch(sector_k, branches, block)
    before = passed_along(rotated, "circ", 1)
    joined = jnp.concatenate([before, rotated], axis=3)
    first_index = edge_count - within - 1
    return lax.dynamic_slice_in_dim(joined, first_index, edge_count + 1, 3)


def project_mortar(incoming, amount, whole_k, is_stator, first_table, second_table):
    highest = lax.Precision.HIGHEST
    window = rotate_window(incoming, amount, whole_k, is_stator)
    edge_count = incoming.shape[-1]
    result = jnp.einsum(
        "mn,rnxe->rmxe", first_table, window[:, :, :, :edge_count], precision=highest
    )
    return result + jnp.einsum(
        "mn,rnxe->rmxe", second_table, window[:, :, :, 1:], precision=highest
    )


def local(field, coeffs, reaction, step_scale, rotation):
    side_index = lax.axis_index("side")
    lower = lax.axis_size("side") // 2 - 1
    cycle_length = field.shape[-1] * lax.axis_size("circ")
    is_stator = side_index > lower
    current = field[0]
    for step in range(STEPS):
        applied = element_apply(current, coeffs[0], reaction[0])
        zero_row = jnp.zeros_like(applied[:, 0, :, :1])
        summed = applied.at[:, 6].add(jnp.concatenate([applied[:, 0, :, 1:], zero_row], axis=2))
        summed = summed.at[:, 0].add(jnp.concatenate([zero_row, applied[:, 6, :, :-1]], axis=2))
        sector_rims = jnp.stack([applied[:, :, 0], applied[:, :, 6]])
        padded = padded_2(sector_rims, (("circ", 4),), 1, True)
        summed = summed.at[:, :, 6].add(padded[0, :, :, :, 2:])
        summed = summed.at[:, :, 0].add(padded[1, :, :, :, :-2])
        axial_faces = jnp.stack([applied[0], applied[6]])
        layered = padded_2(axial_faces, (("side", 0),), 1, False)
        below_top = layered[0]
        above_bottom = layered[3]
        offset = rotation[step]
        whole_k = offset // SUBSTEPS
        fraction = (offset % SUBSTEPS).astype(jnp.float32) / SUBSTEPS
        from_left, from_right = mortar_tables(fraction)
        first_table = jnp.where(is_stator, from_left, from_right.T)
        second_table = jnp.where(is_stator, from_right, from_left.T)
        amount = jnp.where(is_stator, whole_k, cycle_length - whole_k - 1)
        incoming = jnp.where(is_stator, below_top, above_bottom)
        contribution = project_mortar(
            incoming, amount, whole_k, is_stator, first_table, second_table
        )
        bottom_add = jnp.where(side_index == lower + 1, contribution, below_top)
        top_add = jnp.where(side_index == lower, contribution, above_bottom)
        summed = summed.at[0].add(bottom_add)
        summed = summed.at[6].add(top_add)
        current = current - step_scale[0] * summed
    return current[None]


N = 7
MESH = pl.DeviceIdType.MESH
CHUNKS = ((0, 3), (3, 2), (5, 2))


def half_tables(matrix):
    minus = 0.5 * (matrix[:3, :3] - matrix[:3, :3:-1])
    plus = 0.5 * (matrix[:3, :3] + matrix[:3, :3:-1])
    return minus, plus


def weighted(constants, values):
    total = float(constants[0]) * values[0]
    for constant, value in zip(constants[1:], values[1:]):
        total = total + float(constant) * value
    return total


def derivative_of(u):
    table = derivative_table()
    minus, plus = half_tables(table)
    odd = [u[j] - u[6 - j] for j in range(3)]
    twice = u[3] + u[3]
    even = [(u[j] + u[6 - j]) - twice for j in range(3)]
    p = [weighted(minus[i], odd) for i in range(3)]
    q = [weighted(plus[i], even) for i in range(3)]
    middle = weighted(table[3, :3], odd)
    return [p[i] + q[i] for i in range(3)] + [middle] + [p[i] - q[i] for i in (2, 1, 0)]


def transposed_of(w):
    table = derivative_table().T
    minus, plus = half_tables(table)
    odd = [w[j] - w[6 - j] for j in range(3)]
    even = [w[j] + w[6 - j] for j in range(3)] + [w[3]]
    p = [weighted(minus[i], odd) for i in range(3)]
    q = [weighted(list(plus[i]) + [table[i, 3]], even) for i in range(3)]
    middle = -2.0 * (p[0] + p[1] + p[2])
    return [p[i] + q[i] for i in range(3)] + [middle] + [p[i] - q[i] for i in (2, 1, 0)]


def mortar_constants():
    points = gll_points()
    heights = (1.0 + points) * 0.5
    tables = np.zeros((SUBSTEPS, N, N), np.float32)
    on_left = np.zeros((SUBSTEPS, N), np.int32)
    for f in range(SUBSTEPS):
        fraction = f / SUBSTEPS
        for m in range(N):
            left = heights[m] < fraction
            on_left[f, m] = left
            place = 2.0 * (heights[m] - fraction + left) - 1.0
            for n in range(N):
                others = [q for q in range(N) if q != n]
                tables[f, m, n] = np.prod(
                    [(place - points[q]) / (points[n] - points[q]) for q in others]
                )
    return tables.reshape(-1), on_left.reshape(-1)


def rotated(value, shift, lane, sectors):
    width = value.shape[1]
    within = lax.rem(shift, width)
    whole = lax.rem(lax.div(shift, width), sectors)
    turned = pltpu.roll(value, within, 1)
    near = pltpu.roll(turned, whole, 0)
    far = pltpu.roll(near, 1, 0)
    return jnp.where(lane >= within, near, far)


def paired(index, mask, count):
    result, bit = 0, 1
    while bit < count:
        flip = (mask // bit) % 2
        result = result + bit * lax.rem(lax.div(index, bit) + flip, 2)
        bit *= 2
    return result


def step_kernel(
    lower, circ_count, rot_ref, table_ref, left_ref, field_ref, coeffs_ref, reaction_ref,
    scale_ref, out_ref, U, K, R, S, A, G, O, M, C, B, ends, ends_in, load_sem, store_sem,
    conf_send, conf_recv, end_send, end_recv, one_send, one_recv, two_send, two_recv, own_sem,
):
    circ = lax.axis_index("circ")
    side = lax.axis_index("side")
    odd = lax.rem(side, 2)
    conf_a = 6 - 6 * odd
    mort_a = 6 * odd
    mate = side + 1 - 2 * odd
    across = 2 * lower + 1 - side
    at_interface = jnp.logical_or(side == lower, side == lower + 1)
    ahead = lax.rem(circ + 1, circ_count)
    behind = lax.rem(circ + circ_count - 1, circ_count)
    width = U.shape[-1]
    rows = U.shape[-2]
    lane = lax.broadcasted_iota(jnp.int32, (rows, width), 1)
    row = lax.broadcasted_iota(jnp.int32, (rows, width), 0)

    loads = [
        pltpu.make_async_copy(field_ref.at[0], U, load_sem.at[0]),
        pltpu.make_async_copy(reaction_ref.at[0], R, load_sem.at[1]),
        pltpu.make_async_copy(coeffs_ref.at[0, 2], K.at[2], load_sem.at[2]),
        pltpu.make_async_copy(coeffs_ref.at[0, 1], K.at[1], load_sem.at[3]),
        pltpu.make_async_copy(coeffs_ref.at[0, 0], K.at[0], load_sem.at[4]),
        pltpu.make_async_copy(scale_ref.at[0], S, load_sem.at[5]),
    ]
    for load in loads:
        load.start()

    barrier = pltpu.get_barrier_semaphore()
    pl.semaphore_signal(
        barrier, inc=1, device_id={"circ": circ, "side": mate}, device_id_type=MESH
    )

    @pl.when(at_interface)
    def _():
        for d in range(circ_count):
            other = lax.rem(circ + d, circ_count)
            pl.semaphore_signal(
                barrier, inc=1, device_id={"circ": other, "side": across}, device_id_type=MESH
            )
            if d > 0:
                pl.semaphore_signal(
                    barrier, inc=1, device_id={"circ": other, "side": side}, device_id_type=MESH
                )

    @pl.when(jnp.logical_not(at_interface))
    def _():
        for other in (ahead, behind):
            pl.semaphore_signal(
                barrier, inc=1, device_id={"circ": other, "side": side}, device_id_type=MESH
            )

    def barrier_wait():
        @pl.when(at_interface)
        def _():
            pl.semaphore_wait(barrier, 2 * circ_count)

        @pl.when(jnp.logical_not(at_interface))
        def _():
            pl.semaphore_wait(barrier, 3)

    derivative = derivative_table()
    is_odd = odd == 1
    column = [
        jnp.where(is_odd, float(derivative[p, 6]), float(derivative[p, 0])) for p in range(N)
    ]
    square = [
        jnp.where(is_odd, float(derivative[p, 6] ** 2), float(derivative[p, 0] ** 2))
        for p in range(N)
    ]
    planes = [jnp.where(is_odd, 0, N)] + list(range(1, N - 1)) + [jnp.where(is_odd, N, 6)]

    def line(direction, i, j, start=None):
        def at(p):
            return ((p, i, j), (i, p, j), (i, j, p))[direction]

        def to(p):
            return (planes[p], i, j) if direction == 0 else at(p)

        u = [U[at(p)] for p in range(N)]
        g = derivative_of(u)
        w = [g[p] * K[(direction,) + at(p)] for p in range(N)]
        y = transposed_of(w)
        for p in range(N):
            base = A[to(p)] if start is None else start(at(p), u[p])
            A[to(p)] = base + y[p]

    def reacted(at, u):
        return R[at] * u

    def mortar_start(at, u):
        _, r, c = at
        return B[0, r, c] + B[1, r, c] * u

    def circ_lines():
        @pl.loop(0, N - 1)
        def _(q):
            for r in range(N):
                line(2, q + 1 - odd, r, reacted)

    def radial_lines():
        @pl.loop(0, N - 1)
        def _(q):
            for c in range(N):
                line(1, q + 1 - odd, c)

    def partial_axial():
        @pl.loop(0, N)
        def _(r):
            for c in range(N):
                u = [U[p, r, c] for p in range(N)]
                u[0] = jnp.where(is_odd, u[0], 0.0)
                u[6] = jnp.where(is_odd, 0.0, u[6])
                g = derivative_of(u)
                total = column[0] * (g[0] * K[0, 0, r, c])
                for p in range(1, N):
                    total = total + column[p] * (g[p] * K[0, p, r, c])
                B[0, r, c] = total

    for load in loads[:3]:
        load.wait()
    circ_lines()
    loads[3].wait()
    radial_lines()
    loads[4].wait()
    partial_axial()

    @pl.loop(0, N)
    def _(r):
        for c in range(N):
            total = R[mort_a, r, c]
            for p in range(N):
                total = total + square[p] * K[0, p, r, c]
            B[1, r, c] = total

    loads[5].wait()
    barrier_wait()

    def update_plane(a, from_ahead, from_behind, extra):
        for r in range(N):
            i = a * N + r
            for c in range(N):
                s = A[a, r, c]
                if r == 6:
                    s = s + jnp.where(row < rows - 1, pltpu.roll(A[a, 0, c], rows - 1, 0), 0.0)
                if r == 0:
                    s = s + jnp.where(row > 0, pltpu.roll(A[a, 6, c], 1, 0), 0.0)
                if c == 6:
                    s = s + jnp.where(
                        lane == width - 1,
                        pltpu.roll(from_ahead, width - 1 - i, 1),
                        pltpu.roll(A[a, r, 0], width - 1, 1),
                    )
                if c == 0:
                    s = s + jnp.where(
                        lane == 0,
                        pltpu.roll(from_behind, lax.rem(width - i, width), 1),
                        pltpu.roll(A[a, r, 6], 1, 1),
                    )
                if extra is not None:
                    s = s + extra[r, c]
                U[a, r, c] = U[a, r, c] - S[a, r, c] * s

    def one_step(t, _):
        par = lax.rem(t, 2)

        def conf_copy():
            return pltpu.make_async_remote_copy(
                src_ref=A.at[conf_a], dst_ref=C.at[par], send_sem=conf_send,
                recv_sem=conf_recv.at[par], device_id={"circ": circ, "side": mate},
                device_id_type=MESH,
            )

        def end_copy(which, target):
            return pltpu.make_async_remote_copy(
                src_ref=ends.at[which], dst_ref=ends_in.at[par, which],
                send_sem=end_send.at[which], recv_sem=end_recv.at[par, which],
                device_id={"circ": target, "side": side}, device_id_type=MESH,
            )

        def one_copy(h, d):
            rows_of = pl.ds(*CHUNKS[h])
            target = paired(circ, d, circ_count)
            return pltpu.make_async_remote_copy(
                src_ref=A.at[mort_a, rows_of, :, pl.ds(target, 1), :],
                dst_ref=G.at[par, rows_of, :, pl.ds(circ, 1), :],
                send_sem=one_send.at[h, d], recv_sem=one_recv.at[par, h, d],
                device_id={"circ": target, "side": across}, device_id_type=MESH,
            )

        def two_copy(h, d):
            rows_of = pl.ds(*CHUNKS[h])
            target = paired(circ, d, circ_count)
            return pltpu.make_async_remote_copy(
                src_ref=O.at[rows_of, :, pl.ds(target, 1), :],
                dst_ref=M.at[par, rows_of, :, pl.ds(circ, 1), :],
                send_sem=two_send.at[h, d], recv_sem=two_recv.at[par, h, d],
                device_id={"circ": target, "side": side}, device_id_type=MESH,
            )

        def own_copy():
            return pltpu.make_async_copy(
                O.at[:, :, pl.ds(circ, 1), :], M.at[par, :, :, pl.ds(circ, 1), :], own_sem
            )

        for q in range(N):
            line(2, mort_a, q, mortar_start)
        for q in range(N):
            line(1, mort_a, q)

        @pl.when(at_interface)
        def _():
            for h in range(len(CHUNKS)):
                for d in reversed(range(circ_count)):
                    one_copy(h, d).start()

        @pl.loop(0, N)
        def _(r):
            for c in range(N):
                line(0, r, c)

        conf_copy().start()

        def pack(a, carry):
            low, high = carry
            for r in range(N):
                i = a * N + r
                low = jnp.where(lane == i, pltpu.roll(A[a, r, 0], i, 1), low)
                high = jnp.where(lane == i, pltpu.roll(A[a, r, 6], i + 1, 1), high)
            return low, high

        zero = jnp.zeros((rows, width), jnp.float32)
        low, high = lax.fori_loop(0, N, pack, (zero, zero))
        ends[0] = low
        ends[1] = high
        end_copy(0, behind).start()
        end_copy(1, ahead).start()

        offset = rot_ref[t]
        k = lax.div(offset, SUBSTEPS)
        f = offset - SUBSTEPS * k
        cycle = circ_count * width

        def stator_rows(r):
            values = [G[par, r, n] for n in range(N)]
            for m in range(N):
                total = table_ref[f * N * N + m * N] * values[0]
                for n in range(1, N):
                    total = total + table_ref[f * N * N + m * N + n] * values[n]
                O[r, m] = rotated(total, k + left_ref[f * N + m], lane, circ_count)

        def rotor_rows(r):
            values = [
                rotated(G[par, r, m], cycle - k - left_ref[f * N + m], lane, circ_count)
                for m in range(N)
            ]
            for n in range(N):
                total = table_ref[f * N * N + n] * values[0]
                for m in range(1, N):
                    total = total + table_ref[f * N * N + m * N + n] * values[m]
                O[r, n] = total

        for h, (begin, count) in enumerate(CHUNKS):
            @pl.when(at_interface)
            def _():
                for d in range(circ_count):
                    one_copy(h, d).wait_recv()

            @pl.when(side == lower + 1)
            def _():
                pl.loop(begin, begin + count)(stator_rows)

            @pl.when(side == lower)
            def _():
                pl.loop(begin, begin + count)(rotor_rows)

            @pl.when(at_interface)
            def _():
                for d in reversed(range(1, circ_count)):
                    two_copy(h, d).start()

        @pl.when(at_interface)
        def _():
            own_copy().start()

        end_copy(0, behind).wait_recv()
        end_copy(1, ahead).wait_recv()
        from_ahead = ends_in[par, 0]
        from_behind = ends_in[par, 1]

        @pl.loop(1, N - 1)
        def _(a):
            update_plane(a, from_ahead, from_behind, None)

        conf_copy().wait_recv()
        update_plane(conf_a, from_ahead, from_behind, C.at[par])

        conf_copy().wait_send()

        @pl.when(t < STEPS - 1)
        def _():
            circ_lines()
            radial_lines()
            partial_axial()

        @pl.when(t == STEPS - 1)
        def _():
            early_store().start()

        @pl.when(at_interface)
        def _():
            own_copy().wait()
            for h in range(len(CHUNKS)):
                for d in range(1, circ_count):
                    two_copy(h, d).wait_recv()
            update_plane(mort_a, from_ahead, from_behind, M.at[par])
            for h in range(len(CHUNKS)):
                for d in range(circ_count):
                    one_copy(h, d).wait_send()
                for d in range(1, circ_count):
                    two_copy(h, d).wait_send()

        @pl.when(jnp.logical_not(at_interface))
        def _():
            update_plane(mort_a, from_ahead, from_behind, None)

        end_copy(0, behind).wait_send()
        end_copy(1, ahead).wait_send()
        return 0

    def early_store():
        others = pl.ds(1 - odd, N - 1)
        return pltpu.make_async_copy(U.at[others], out_ref.at[0, others], store_sem.at[0])

    lax.fori_loop(0, STEPS, one_step, 0)
    late = pltpu.make_async_copy(U.at[mort_a], out_ref.at[0, mort_a], store_sem.at[1])
    late.start()
    early_store().wait()
    late.wait()


def fused(mesh, field, coeffs, reaction, step_scale, rotation):
    circ_count = mesh.shape["circ"]
    lower = mesh.shape["side"] // 2 - 1
    node_shape = field.shape[1:]
    face_shape = node_shape[1:]
    tile = face_shape[2:]
    tables, on_left = mortar_constants()
    smem = pl.BlockSpec(memory_space=pltpu.SMEM)
    anywhere = pl.BlockSpec(memory_space=pl.ANY)
    dma = pltpu.SemaphoreType.DMA
    f32 = jnp.float32
    return pl.pallas_call(
        partial(step_kernel, lower, circ_count),
        out_shape=jax.ShapeDtypeStruct(field.shape, f32),
        in_specs=[smem, smem, smem] + [anywhere] * 4,
        out_specs=anywhere,
        scratch_shapes=[
            pltpu.VMEM(node_shape, f32),
            pltpu.VMEM(coeffs.shape[1:], f32),
            pltpu.VMEM(node_shape, f32),
            pltpu.VMEM(node_shape, f32),
            pltpu.VMEM((N + 1,) + face_shape, f32),
            pltpu.VMEM((2,) + face_shape, f32),
            pltpu.VMEM(face_shape, f32),
            pltpu.VMEM((2,) + face_shape, f32),
            pltpu.VMEM((2,) + face_shape, f32),
            pltpu.VMEM((2,) + face_shape, f32),
            pltpu.VMEM((2,) + tile, f32),
            pltpu.VMEM((2, 2) + tile, f32),
            dma((6,)),
            dma((2,)),
            dma(()),
            dma((2,)),
            dma((2,)),
            dma((2, 2)),
            dma((len(CHUNKS), circ_count)),
            dma((2, len(CHUNKS), circ_count)),
            dma((len(CHUNKS), circ_count)),
            dma((2, len(CHUNKS), circ_count)),
            dma(()),
        ],
        compiler_params=pltpu.CompilerParams(collective_id=0, has_side_effects=True),
    )(rotation, jnp.asarray(tables), jnp.asarray(on_left), field, coeffs, reaction, step_scale)


def solution(mesh):
    def body(field, coeffs, reaction, step_scale, rotation):
        radial_count, lanes = field.shape[-2:]
        whole_circle = radial_count == mesh.shape["circ"] == 8 and lanes == 128
        if whole_circle and mesh.shape["side"] == 4:
            return fused(mesh, field, coeffs, reaction, step_scale, rotation)
        return local(field, coeffs, reaction, step_scale, rotation)

    in_specs = (
        P("side", None, None, None, None, "circ"),
        P("side", None, None, None, None, None, "circ"),
        P("side", None, None, None, None, "circ"),
        P("side", None, None, None, None, "circ"),
        P(),
    )
    out_specs = P("side", None, None, None, None, "circ")
    return jax.shard_map(body, mesh=mesh, in_specs=in_specs, out_specs=out_specs, check_vma=False)
```

```python
from functools import partial

import jax
import jax.numpy as jnp
import numpy as np
from jax import lax
from jax.experimental import pallas as pl
from jax.experimental.pallas import tpu as pltpu
from jax.sharding import PartitionSpec as P

SUBSTEPS = 3
STEPS = 4


def passed_along(value, axis, steps):
    count = lax.axis_size(axis)
    pairs = [(source, (source + steps) % count) for source in range(count)]
    return lax.ppermute(value, axis, pairs)


def padded_2(block, sides, width, periodic):
    for axis, dim in sides:
        count = lax.axis_size(axis)
        forward = [(i, i + 1) for i in range(count - 1)]
        if periodic:
            forward.append((count - 1, 0))
        backward = [(target, source) for source, target in forward]
        low = lax.ppermute(
            lax.slice_in_dim(block, block.shape[dim] - width, None, axis=dim), axis, forward
        )
        high = lax.ppermute(lax.slice_in_dim(block, 0, width, axis=dim), axis, backward)
        block = jnp.concatenate([low, block, high], axis=dim)
    return block


def gll_points():
    return np.array(
        [
            -1.0,
            -0.830223896278567,
            -0.4688487934707142,
            0.0,
            0.4688487934707142,
            0.830223896278567,
            1.0,
        ]
    )


def derivative_table():
    points = gll_points()
    node_count = points.shape[0]
    weights = np.array(
        [
            1.0 / np.prod([points[j] - points[k] for k in range(node_count) if k != j])
            for j in range(node_count)
        ]
    )
    derivative = np.zeros((node_count, node_count))
    for i in range(node_count):
        for j in range(node_count):
            if i != j:
                derivative[i, j] = weights[j] / weights[i] / (points[i] - points[j])
        derivative[i, i] = -np.sum(derivative[i])
    return derivative


def lagrange_rows(locations):
    points = gll_points()
    identity_mask = np.eye(7) > 0.5
    differences = np.array(
        [[1.0 if q == n else points[n] - points[q] for q in range(7)] for n in range(7)]
    )
    denominator = np.prod(differences, axis=1)
    distances = locations[:, None] - jnp.asarray(points, jnp.float32)[None, :]
    factors = jnp.where(identity_mask[None, :, :], 1.0, distances[:, None, :])
    return jnp.prod(factors, axis=2) / jnp.asarray(denominator, jnp.float32)[None, :]


def mortar_tables(fraction):
    heights = (1.0 + jnp.asarray(gll_points(), jnp.float32)) * 0.5
    on_right = heights >= fraction
    shifted_height = jnp.where(on_right, heights - fraction, heights - fraction + 1.0)
    values = lagrange_rows(2.0 * shifted_height - 1.0)
    from_right = jnp.where(on_right[:, None], values, 0.0)
    from_left = jnp.where(on_right[:, None], 0.0, values)
    return (from_left, from_right)


def element_apply(field, coeffs, reaction):
    derivative = jnp.asarray(derivative_table(), jnp.float32)
    highest = lax.Precision.HIGHEST
    grad_axial = jnp.einsum("pa,arcxe->prcxe", derivative, field, precision=highest)
    grad_radial = jnp.einsum("pr,arcxe->apcxe", derivative, field, precision=highest)
    grad_circ = jnp.einsum("pc,arcxe->arpxe", derivative, field, precision=highest)
    result = reaction * field
    result = result + jnp.einsum(
        "pa,prcxe->arcxe", derivative, coeffs[0] * grad_axial, precision=highest
    )
    result = result + jnp.einsum(
        "pr,apcxe->arcxe", derivative, coeffs[1] * grad_radial, precision=highest
    )
    result = result + jnp.einsum(
        "pc,arpxe->arcxe", derivative, coeffs[2] * grad_circ, precision=highest
    )
    return result


def fixed_pair(hops, circ_count, is_stator, data):
    ahead = passed_along(data, "circ", hops)
    behind = passed_along(data, "circ", (circ_count - hops - 1) % circ_count)
    return jnp.where(is_stator, ahead, behind)


def rotate_window(block, amount, whole_k, is_stator):
    edge_count = block.shape[-1]
    circ_count = lax.axis_size("circ")
    within = amount % edge_count
    sector_k = whole_k // edge_count
    branches = [partial(fixed_pair, hops, circ_count, is_stator) for hops in range(circ_count)]
    rotated = lax.switch(sector_k, branches, block)
    before = passed_along(rotated, "circ", 1)
    joined = jnp.concatenate([before, rotated], axis=3)
    first_index = edge_count - within - 1
    return lax.dynamic_slice_in_dim(joined, first_index, edge_count + 1, 3)


def project_mortar(incoming, amount, whole_k, is_stator, first_table, second_table):
    highest = lax.Precision.HIGHEST
    window = rotate_window(incoming, amount, whole_k, is_stator)
    edge_count = incoming.shape[-1]
    result = jnp.einsum(
        "mn,rnxe->rmxe", first_table, window[:, :, :, :edge_count], precision=highest
    )
    return result + jnp.einsum(
        "mn,rnxe->rmxe", second_table, window[:, :, :, 1:], precision=highest
    )


def local(field, coeffs, reaction, step_scale, rotation):
    side_index = lax.axis_index("side")
    lower = lax.axis_size("side") // 2 - 1
    cycle_length = field.shape[-1] * lax.axis_size("circ")
    is_stator = side_index > lower
    current = field[0]
    for step in range(STEPS):
        applied = element_apply(current, coeffs[0], reaction[0])
        zero_row = jnp.zeros_like(applied[:, 0, :, :1])
        summed = applied.at[:, 6].add(jnp.concatenate([applied[:, 0, :, 1:], zero_row], axis=2))
        summed = summed.at[:, 0].add(jnp.concatenate([zero_row, applied[:, 6, :, :-1]], axis=2))
        sector_rims = jnp.stack([applied[:, :, 0], applied[:, :, 6]])
        padded = padded_2(sector_rims, (("circ", 4),), 1, True)
        summed = summed.at[:, :, 6].add(padded[0, :, :, :, 2:])
        summed = summed.at[:, :, 0].add(padded[1, :, :, :, :-2])
        axial_faces = jnp.stack([applied[0], applied[6]])
        layered = padded_2(axial_faces, (("side", 0),), 1, False)
        below_top = layered[0]
        above_bottom = layered[3]
        offset = rotation[step]
        whole_k = offset // SUBSTEPS
        fraction = (offset % SUBSTEPS).astype(jnp.float32) / SUBSTEPS
        from_left, from_right = mortar_tables(fraction)
        first_table = jnp.where(is_stator, from_left, from_right.T)
        second_table = jnp.where(is_stator, from_right, from_left.T)
        amount = jnp.where(is_stator, whole_k, cycle_length - whole_k - 1)
        incoming = jnp.where(is_stator, below_top, above_bottom)
        contribution = project_mortar(
            incoming, amount, whole_k, is_stator, first_table, second_table
        )
        bottom_add = jnp.where(side_index == lower + 1, contribution, below_top)
        top_add = jnp.where(side_index == lower, contribution, above_bottom)
        summed = summed.at[0].add(bottom_add)
        summed = summed.at[6].add(top_add)
        current = current - step_scale[0] * summed
    return current[None]


N = 7
MESH = pl.DeviceIdType.MESH
CHUNKS = ((0, 3), (3, 4))
RIMS = (0, 6)
INNER = (1, 2, 3, 4, 5)
FAR_FIRST = (5, 4, 7, 6, 3, 2, 1, 0)


def half_tables(matrix):
    minus = 0.5 * (matrix[:3, :3] - matrix[:3, :3:-1])
    plus = 0.5 * (matrix[:3, :3] + matrix[:3, :3:-1])
    return minus, plus


def weighted(constants, values):
    total = float(constants[0]) * values[0]
    for constant, value in zip(constants[1:], values[1:]):
        total = total + float(constant) * value
    return total


def derivative_of(u):
    table = derivative_table()
    minus, plus = half_tables(table)
    odd = [u[j] - u[6 - j] for j in range(3)]
    twice = u[3] + u[3]
    even = [(u[j] + u[6 - j]) - twice for j in range(3)]
    p = [weighted(minus[i], odd) for i in range(3)]
    q = [weighted(plus[i], even) for i in range(3)]
    middle = weighted(table[3, :3], odd)
    return [p[i] + q[i] for i in range(3)] + [middle] + [p[i] - q[i] for i in (2, 1, 0)]


def transposed_of(w):
    table = derivative_table().T
    minus, plus = half_tables(table)
    odd = [w[j] - w[6 - j] for j in range(3)]
    even = [w[j] + w[6 - j] for j in range(3)] + [w[3]]
    p = [weighted(minus[i], odd) for i in range(3)]
    q = [weighted(list(plus[i]) + [table[i, 3]], even) for i in range(3)]
    middle = -2.0 * (p[0] + p[1] + p[2])
    return [p[i] + q[i] for i in range(3)] + [middle] + [p[i] - q[i] for i in (2, 1, 0)]


def mortar_constants():
    points = gll_points()
    heights = (1.0 + points) * 0.5
    tables = np.zeros((SUBSTEPS, N, N), np.float32)
    on_left = np.zeros((SUBSTEPS, N), np.int32)
    for f in range(SUBSTEPS):
        fraction = f / SUBSTEPS
        for m in range(N):
            left = heights[m] < fraction
            on_left[f, m] = left
            place = 2.0 * (heights[m] - fraction + left) - 1.0
            for n in range(N):
                others = [q for q in range(N) if q != n]
                tables[f, m, n] = np.prod(
                    [(place - points[q]) / (points[n] - points[q]) for q in others]
                )
    return tables.reshape(-1), on_left.reshape(-1)


def rotated(value, shift, lane, sectors):
    width = value.shape[1]
    within = lax.rem(shift, width)
    whole = lax.rem(lax.div(shift, width), sectors)
    turned = pltpu.roll(value, within, 1)
    near = pltpu.roll(turned, whole, 0)
    far = pltpu.roll(near, 1, 0)
    return jnp.where(lane >= within, near, far)


def paired(index, mask, count):
    result, bit = 0, 1
    while bit < count:
        flip = (mask // bit) % 2
        result = result + bit * lax.rem(lax.div(index, bit) + flip, 2)
        bit *= 2
    return result


def step_kernel(
    lower, circ_count, first, workers, work_sides, rot_ref, table_ref, left_ref, field_ref,
    coeffs_ref, reaction_ref, scale_ref, out_ref, K, R, S, A, G, O, M, C, B, ends, ends_in,
    load_sem, conf_send, conf_recv, end_send, end_recv, one_send, one_recv, two_send, two_recv,
):
    U = out_ref.at[0]
    circ = lax.axis_index("circ")
    side = lax.axis_index("side")
    odd = lax.rem(side, 2)
    conf_a = 6 - 6 * odd
    mort_a = 6 * odd
    mate = side + 1 - 2 * odd
    at_interface = jnp.logical_or(side == lower, side == lower + 1)
    own_way = jnp.where(side == lower, 0, 1)
    central = jnp.logical_and(circ >= first, circ < first + workers)
    is_worker, side_place = [], []
    for sides in work_sides:
        is_here = side == sides[0]
        place = 0
        for i in range(1, len(sides)):
            is_here = jnp.logical_or(is_here, side == sides[i])
            place = place + jnp.where(side == sides[i], i, 0)
        is_worker.append(jnp.logical_and(central, is_here))
        side_place.append(place)
    slots = G.shape[1]
    locals_count = G.shape[2]
    near = 2 * lax.div(circ, circ_count // 2) + lax.rem(circ, 2)
    ahead = lax.rem(circ + 1, circ_count)
    behind = lax.rem(circ + circ_count - 1, circ_count)
    width = U.shape[-1]
    rows = U.shape[-2]
    lane = lax.broadcasted_iota(jnp.int32, (rows, width), 1)
    row = lax.broadcasted_iota(jnp.int32, (rows, width), 0)

    others = pl.ds(1 - odd, N - 1)
    face_loads = [
        pltpu.make_async_copy(field_ref.at[0], U, load_sem.at[0]),
        pltpu.make_async_copy(coeffs_ref.at[0, 0], K.at[0], load_sem.at[1]),
        pltpu.make_async_copy(reaction_ref.at[0, mort_a], R.at[mort_a], load_sem.at[2]),
        pltpu.make_async_copy(coeffs_ref.at[0, 1, mort_a], K.at[1, mort_a], load_sem.at[3]),
        pltpu.make_async_copy(coeffs_ref.at[0, 2, mort_a], K.at[2, mort_a], load_sem.at[4]),
    ]
    later_loads = [
        pltpu.make_async_copy(reaction_ref.at[0, others], R.at[others], load_sem.at[5]),
        pltpu.make_async_copy(coeffs_ref.at[0, 1, others], K.at[1, others], load_sem.at[6]),
        pltpu.make_async_copy(coeffs_ref.at[0, 2, others], K.at[2, others], load_sem.at[7]),
        pltpu.make_async_copy(scale_ref.at[0], S, load_sem.at[8]),
    ]
    for load in face_loads + later_loads:
        load.start()

    barrier = pltpu.get_barrier_semaphore()
    pl.semaphore_signal(
        barrier, inc=1, device_id={"circ": circ, "side": mate}, device_id_type=MESH
    )

    def greet(other_circ, other_side, when):
        same = jnp.logical_and(circ == other_circ, side == other_side)

        @pl.when(jnp.logical_and(when, jnp.logical_not(same)))
        def _():
            pl.semaphore_signal(
                barrier, inc=1, device_id={"circ": other_circ, "side": other_side},
                device_id_type=MESH,
            )

    greeted = 3
    for other in (ahead, behind):
        pl.semaphore_signal(
            barrier, inc=1, device_id={"circ": other, "side": side}, device_id_type=MESH
        )
    for way, sides in enumerate(work_sides):
        meets_self = jnp.logical_and(at_interface, is_worker[way]).astype(jnp.int32)
        for work_side in sides:
            for w in range(first, first + workers):
                greet(w, work_side, at_interface)
        for c in range(circ_count):
            for face_side in (lower, lower + 1):
                greet(c, face_side, is_worker[way])
        greeted = greeted + jnp.where(at_interface, workers * len(sides), 0) - meets_self
        greeted = greeted + jnp.where(is_worker[way], 2 * circ_count, 0) - meets_self

    def barrier_wait():
        pl.semaphore_wait(barrier, greeted)

    derivative = derivative_table()
    is_odd = odd == 1
    column = [
        jnp.where(is_odd, float(derivative[p, 6]), float(derivative[p, 0])) for p in range(N)
    ]
    square = [
        jnp.where(is_odd, float(derivative[p, 6] ** 2), float(derivative[p, 0] ** 2))
        for p in range(N)
    ]
    planes = [jnp.where(is_odd, 0, N)] + list(range(1, N - 1)) + [jnp.where(is_odd, N, 6)]

    def line(direction, i, j, start=None):
        def at(p):
            return ((p, i, j), (i, p, j), (i, j, p))[direction]

        def to(p):
            return (planes[p], i, j) if direction == 0 else at(p)

        u = [U[at(p)] for p in range(N)]
        g = derivative_of(u)
        w = [g[p] * K[(direction,) + at(p)] for p in range(N)]
        y = transposed_of(w)
        for p in range(N):
            base = A[to(p)] if start is None else start(at(p), u[p])
            A[to(p)] = base + y[p]

    def reacted(at, u):
        return R[at] * u

    def mortar_start(at, u):
        _, r, c = at
        return B[0, r, c] + B[1, r, c] * u

    def circ_lines(plane):
        for r in range(N):
            line(2, plane, r)

    def radial_lines(plane, columns):
        for c in columns:
            line(1, plane, c, reacted)

    def partial_axial(columns):
        @pl.loop(0, N)
        def _(r):
            for c in columns:
                u = [U[p, r, c] for p in range(N)]
                u[0] = jnp.where(is_odd, u[0], 0.0)
                u[6] = jnp.where(is_odd, 0.0, u[6])
                g = derivative_of(u)
                total = column[0] * (g[0] * K[0, 0, r, c])
                for p in range(1, N):
                    total = total + column[p] * (g[p] * K[0, p, r, c])
                B[0, r, c] = total

    def first_lines():
        for load in later_loads[:2]:
            load.wait()

        @pl.loop(0, N - 1)
        def _(q):
            radial_lines(q + 1 - odd, range(N))

        later_loads[2].wait()

        @pl.loop(0, N - 1)
        def _(q):
            circ_lines(q + 1 - odd)

        later_loads[3].wait()

    for load in face_loads:
        load.wait()
    partial_axial(range(N))

    @pl.loop(0, N)
    def _(r):
        for c in range(N):
            total = R[mort_a, r, c]
            for p in range(N):
                total = total + square[p] * K[0, p, r, c]
            B[1, r, c] = total

    barrier_wait()

    def update_plane(a, columns, from_ahead, from_behind, extra):
        for r in range(N):
            i = a * N + r
            for c in columns:
                s = A[a, r, c]
                if r == 6:
                    s = s + jnp.where(row < rows - 1, pltpu.roll(A[a, 0, c], rows - 1, 0), 0.0)
                if r == 0:
                    s = s + jnp.where(row > 0, pltpu.roll(A[a, 6, c], 1, 0), 0.0)
                if c == 6:
                    s = s + jnp.where(
                        lane == width - 1,
                        pltpu.roll(from_ahead, width - 1 - i, 1),
                        pltpu.roll(A[a, r, 0], width - 1, 1),
                    )
                if c == 0:
                    s = s + jnp.where(
                        lane == 0,
                        pltpu.roll(from_behind, lax.rem(width - i, width), 1),
                        pltpu.roll(A[a, r, 6], 1, 1),
                    )
                if extra is not None:
                    s = s + extra[r, c]
                U[a, r, c] = U[a, r, c] - S[a, r, c] * s

    def one_step(t, _):
        par = lax.rem(t, 2)

        def conf_copy():
            return pltpu.make_async_remote_copy(
                src_ref=A.at[conf_a], dst_ref=C.at[par], send_sem=conf_send,
                recv_sem=conf_recv.at[par], device_id={"circ": circ, "side": mate},
                device_id_type=MESH,
            )

        def end_copy(which, target):
            return pltpu.make_async_remote_copy(
                src_ref=ends.at[which], dst_ref=ends_in.at[par, which],
                send_sem=end_send.at[which], recv_sem=end_recv.at[par, which],
                device_id={"circ": target, "side": side}, device_id_type=MESH,
            )

        def remote(src, dst, send_sem, recv_sem, to_circ, to_side):
            return pltpu.make_async_remote_copy(
                src_ref=src, dst_ref=dst, send_sem=send_sem, recv_sem=recv_sem,
                device_id={"circ": to_circ, "side": to_side}, device_id_type=MESH,
            )

        def start(src, dst, send_sem, recv_sem, to_circ, to_side, can_be_here):
            copy = remote(src, dst, send_sem, recv_sem, to_circ, to_side)
            if not can_be_here:
                copy.start()
                return
            here = jnp.logical_and(to_circ == circ, to_side == side)

            @pl.when(jnp.logical_not(here))
            def _():
                copy.start()

            @pl.when(here)
            def _():
                pltpu.make_async_copy(src, dst, recv_sem).start()

        def wait_sent(sent, send_sem, one_here):
            def wait(ref):
                remote(ref, ref, send_sem, send_sem, circ, mate).wait_send()

            @pl.when(one_here)
            def _():
                wait(sent.at[..., pl.ds(0, rows - 1), :])

            @pl.when(jnp.logical_not(one_here))
            def _():
                wait(sent)

        def arrived(ref, recv_sem):
            remote(ref, ref, recv_sem, recv_sem, circ, mate).wait_recv()

        own_slot = own_way if slots > 1 else 0

        def start_one(h, d):
            rows_of = pl.ds(*CHUNKS[h])
            place = paired(near, d % workers, workers)
            group = d // workers
            at = group % len(work_sides[0])
            start(
                A.at[mort_a, rows_of, :, pl.ds(group * workers + place, 1), :],
                G.at[par, own_slot, group // len(work_sides[0]), rows_of, :, pl.ds(circ, 1), :],
                one_send, one_recv.at[par, h, own_slot], first + place,
                jnp.where(side == lower, work_sides[0][at], work_sides[1][at]),
                d % workers == 0 and any(lower + w == work_sides[w][at] for w in range(2)),
            )

        def start_two(way, h, j, d):
            rows_of = pl.ds(*CHUNKS[h])
            target = paired(circ, d, circ_count)
            slot = way if slots > 1 else 0
            place = (j * len(work_sides[way]) + side_place[way]) * workers + circ - first
            start(
                O.at[slot, j, rows_of, :, pl.ds(target, 1), :],
                M.at[par, rows_of, :, pl.ds(place, 1), :],
                two_send.at[slot], two_recv.at[par, h], target, lower + 1 - way,
                d == 0 and lower + 1 - way in work_sides[way],
            )

        for q in range(N):
            line(1, mort_a, q, mortar_start)
        for h, (begin, count) in enumerate(CHUNKS):
            for q in range(begin, begin + count):
                line(2, mort_a, q)

            @pl.when(at_interface)
            def _():
                for d in reversed(range(circ_count)):
                    start_one(h, d)

        @pl.when(t == 0)
        def _():
            first_lines()

        def axial_lines(columns):
            @pl.loop(0, N)
            def _(r):
                for c in columns:
                    line(0, r, c)

        axial_lines(RIMS)
        low = jnp.zeros((rows, width), jnp.float32)
        high = low
        for i in range(N * N):
            low = jnp.where(lane == i, pltpu.roll(A[i // N, i % N, 0], i, 1), low)
            high = jnp.where(lane == i, pltpu.roll(A[i // N, i % N, 6], i + 1, 1), high)
        ends[0] = low
        ends[1] = high
        end_copy(0, behind).start()
        end_copy(1, ahead).start()
        axial_lines(INNER)
        conf_copy().start()

        def inner_plane(a, extra):
            update_plane(a, INNER, None, None, extra)

            @pl.when(t < STEPS - 1)
            def _():
                radial_lines(a, INNER)

        @pl.loop(1, N - 1)
        def _(a):
            inner_plane(a, None)

        conf_copy().wait_recv()
        conf_copy().wait_send()
        inner_plane(conf_a, C.at[par])

        @pl.when(t < STEPS - 1)
        def _():
            partial_axial(INNER)

        offset = rot_ref[t]
        k = lax.div(offset, SUBSTEPS)
        f = offset - SUBSTEPS * k
        cycle = circ_count * width

        def stator_rows(slot, places):
            values = [[G[par, slot, j, r, n] for n in range(N)] for j, r in places]
            for m in range(N):
                factors = [table_ref[f * N * N + m * N + n] for n in range(N)]
                shift = k + left_ref[f * N + m]
                for (j, r), own in zip(places, values):
                    total = factors[0] * own[0]
                    for n in range(1, N):
                        total = total + factors[n] * own[n]
                    O[slot, j, r, m] = rotated(total, shift, lane, circ_count)

        def rotor_rows(slot, places):
            shifts = [cycle - k - left_ref[f * N + m] for m in range(N)]
            values = [
                [rotated(G[par, slot, j, r, m], shifts[m], lane, circ_count) for m in range(N)]
                for j, r in places
            ]
            for n in range(N):
                factors = [table_ref[f * N * N + m * N + n] for m in range(N)]
                for (j, r), own in zip(places, values):
                    total = factors[0] * own[0]
                    for m in range(1, N):
                        total = total + factors[m] * own[m]
                    O[slot, j, r, n] = total

        for h, (begin, count) in enumerate(CHUNKS):
            for way, project in enumerate((stator_rows, rotor_rows)):
                @pl.when(is_worker[way])
                def _():
                    slot = way if slots > 1 else 0
                    arrived(G.at[par, slot, :, pl.ds(begin, count)], one_recv.at[par, h, slot])
                    for j in range(locals_count):
                        project(slot, [(j, r) for r in range(begin, begin + count)])
                        for d in FAR_FIRST:
                            start_two(way, h, j, d)

        end_copy(0, behind).wait_recv()
        end_copy(1, ahead).wait_recv()
        from_ahead = ends_in[par, 0]
        from_behind = ends_in[par, 1]

        def rim_plane(a, extra):
            update_plane(a, RIMS, from_ahead, from_behind, extra)

            @pl.when(t < STEPS - 1)
            def _():
                radial_lines(a, RIMS)
                circ_lines(a)

        @pl.loop(1, N - 1)
        def _(a):
            rim_plane(a, None)

        rim_plane(conf_a, C.at[par])

        @pl.when(t < STEPS - 1)
        def _():
            partial_axial(RIMS)

        @pl.when(at_interface)
        def _():
            for h in range(len(CHUNKS)):
                arrived(M.at[par, pl.ds(*CHUNKS[h])], two_recv.at[par, h])
            update_plane(mort_a, range(N), from_ahead, from_behind, M.at[par])
            to_self = False
            for way in range(2):
                if lower + way in work_sides[way]:
                    to_self = jnp.logical_or(
                        to_self, jnp.logical_and(is_worker[way], own_way == way)
                    )
            wait_sent(A.at[mort_a], one_send, jnp.asarray(to_self))

        for way in range(2):
            @pl.when(is_worker[way])
            def _():
                slot = way if slots > 1 else 0
                wait_sent(O.at[slot], two_send.at[slot], side == lower + 1 - way)

        @pl.when(jnp.logical_not(at_interface))
        def _():
            update_plane(mort_a, range(N), from_ahead, from_behind, None)

        end_copy(0, behind).wait_send()
        end_copy(1, ahead).wait_send()
        return 0

    lax.fori_loop(0, STEPS, one_step, 0)


def placed_work(circ_count, lower):
    return circ_count // 4, circ_count // 2, ((lower, lower + 2), (lower, lower + 2))


def fused(mesh, field, coeffs, reaction, step_scale, rotation):
    circ_count = mesh.shape["circ"]
    lower = mesh.shape["side"] // 2 - 1
    first, workers, work_sides = placed_work(circ_count, lower)
    kinds = len(set(work_sides[0]) & set(work_sides[1])) > 0
    slots = 2 if kinds else 1
    rows_each = circ_count // (workers * len(work_sides[0]))
    node_shape = field.shape[1:]
    face_shape = node_shape[1:]
    tile = face_shape[2:]
    tables, on_left = mortar_constants()
    smem = pl.BlockSpec(memory_space=pltpu.SMEM)
    anywhere = pl.BlockSpec(memory_space=pl.ANY)
    dma = pltpu.SemaphoreType.DMA
    f32 = jnp.float32
    operands = (
        rotation, jnp.asarray(tables), jnp.asarray(on_left), field, coeffs, reaction, step_scale
    )
    return pl.pallas_call(
        partial(step_kernel, lower, circ_count, first, workers, work_sides),
        out_shape=jax.ShapeDtypeStruct(field.shape, f32),
        in_specs=[smem, smem, smem] + [anywhere] * 4,
        out_specs=pl.BlockSpec(memory_space=pltpu.VMEM),
        scratch_shapes=[
            pltpu.VMEM(coeffs.shape[1:], f32),
            pltpu.VMEM(node_shape, f32),
            pltpu.VMEM(node_shape, f32),
            pltpu.VMEM((N + 1,) + face_shape, f32),
            pltpu.VMEM((2, slots, rows_each) + face_shape, f32),
            pltpu.VMEM((slots, rows_each) + face_shape, f32),
            pltpu.VMEM((2,) + face_shape, f32),
            pltpu.VMEM((2,) + face_shape, f32),
            pltpu.VMEM((2,) + face_shape, f32),
            pltpu.VMEM((2,) + tile, f32),
            pltpu.VMEM((2, 2) + tile, f32),
            dma((9,)),
            dma(()),
            dma((2,)),
            dma((2,)),
            dma((2, 2)),
            dma(()),
            dma((2, len(CHUNKS), slots)),
            dma((slots,)),
            dma((2, len(CHUNKS))),
        ],
        compiler_params=pltpu.CompilerParams(
            collective_id=0, has_side_effects=True, vmem_limit_bytes=24 * 2**20
        ),
    )(*[pltpu.with_memory_space_constraint(operand, pltpu.HBM) for operand in operands])


def solution(mesh):
    def body(field, coeffs, reaction, step_scale, rotation):
        radial_count, lanes = field.shape[-2:]
        whole_circle = radial_count == mesh.shape["circ"] == 8 and lanes == 128
        if whole_circle and mesh.shape["side"] == 4:
            return fused(mesh, field, coeffs, reaction, step_scale, rotation)
        return local(field, coeffs, reaction, step_scale, rotation)

    in_specs = (
        P("side", None, None, None, None, "circ"),
        P("side", None, None, None, None, None, "circ"),
        P("side", None, None, None, None, "circ"),
        P("side", None, None, None, None, "circ"),
        P(),
    )
    out_specs = P("side", None, None, None, None, "circ")
    return jax.shard_map(body, mesh=mesh, in_specs=in_specs, out_specs=out_specs, check_vma=False)
```

```python
from functools import partial

import jax
import jax.numpy as jnp
import numpy as np
from jax import lax
from jax.experimental import pallas as pl
from jax.experimental.pallas import tpu as pltpu
from jax.sharding import PartitionSpec as P

SUBSTEPS = 3
STEPS = 4


def passed_along(value, axis, steps):
    count = lax.axis_size(axis)
    pairs = [(source, (source + steps) % count) for source in range(count)]
    return lax.ppermute(value, axis, pairs)


def padded_2(block, sides, width, periodic):
    for axis, dim in sides:
        count = lax.axis_size(axis)
        forward = [(i, i + 1) for i in range(count - 1)]
        if periodic:
            forward.append((count - 1, 0))
        backward = [(target, source) for source, target in forward]
        low = lax.ppermute(
            lax.slice_in_dim(block, block.shape[dim] - width, None, axis=dim), axis, forward
        )
        high = lax.ppermute(lax.slice_in_dim(block, 0, width, axis=dim), axis, backward)
        block = jnp.concatenate([low, block, high], axis=dim)
    return block


def gll_points():
    return np.array(
        [
            -1.0,
            -0.830223896278567,
            -0.4688487934707142,
            0.0,
            0.4688487934707142,
            0.830223896278567,
            1.0,
        ]
    )


def derivative_table():
    points = gll_points()
    node_count = points.shape[0]
    weights = np.array(
        [
            1.0 / np.prod([points[j] - points[k] for k in range(node_count) if k != j])
            for j in range(node_count)
        ]
    )
    derivative = np.zeros((node_count, node_count))
    for i in range(node_count):
        for j in range(node_count):
            if i != j:
                derivative[i, j] = weights[j] / weights[i] / (points[i] - points[j])
        derivative[i, i] = -np.sum(derivative[i])
    return derivative


def lagrange_rows(locations):
    points = gll_points()
    identity_mask = np.eye(7) > 0.5
    differences = np.array(
        [[1.0 if q == n else points[n] - points[q] for q in range(7)] for n in range(7)]
    )
    denominator = np.prod(differences, axis=1)
    distances = locations[:, None] - jnp.asarray(points, jnp.float32)[None, :]
    factors = jnp.where(identity_mask[None, :, :], 1.0, distances[:, None, :])
    return jnp.prod(factors, axis=2) / jnp.asarray(denominator, jnp.float32)[None, :]


def mortar_tables(fraction):
    heights = (1.0 + jnp.asarray(gll_points(), jnp.float32)) * 0.5
    on_right = heights >= fraction
    shifted_height = jnp.where(on_right, heights - fraction, heights - fraction + 1.0)
    values = lagrange_rows(2.0 * shifted_height - 1.0)
    from_right = jnp.where(on_right[:, None], values, 0.0)
    from_left = jnp.where(on_right[:, None], 0.0, values)
    return (from_left, from_right)


def element_apply(field, coeffs, reaction):
    derivative = jnp.asarray(derivative_table(), jnp.float32)
    highest = lax.Precision.HIGHEST
    grad_axial = jnp.einsum("pa,arcxe->prcxe", derivative, field, precision=highest)
    grad_radial = jnp.einsum("pr,arcxe->apcxe", derivative, field, precision=highest)
    grad_circ = jnp.einsum("pc,arcxe->arpxe", derivative, field, precision=highest)
    result = reaction * field
    result = result + jnp.einsum(
        "pa,prcxe->arcxe", derivative, coeffs[0] * grad_axial, precision=highest
    )
    result = result + jnp.einsum(
        "pr,apcxe->arcxe", derivative, coeffs[1] * grad_radial, precision=highest
    )
    result = result + jnp.einsum(
        "pc,arpxe->arcxe", derivative, coeffs[2] * grad_circ, precision=highest
    )
    return result


def fixed_pair(hops, circ_count, is_stator, data):
    ahead = passed_along(data, "circ", hops)
    behind = passed_along(data, "circ", (circ_count - hops - 1) % circ_count)
    return jnp.where(is_stator, ahead, behind)


def rotate_window(block, amount, whole_k, is_stator):
    edge_count = block.shape[-1]
    circ_count = lax.axis_size("circ")
    within = amount % edge_count
    sector_k = whole_k // edge_count
    branches = [partial(fixed_pair, hops, circ_count, is_stator) for hops in range(circ_count)]
    rotated = lax.switch(sector_k, branches, block)
    before = passed_along(rotated, "circ", 1)
    joined = jnp.concatenate([before, rotated], axis=3)
    first_index = edge_count - within - 1
    return lax.dynamic_slice_in_dim(joined, first_index, edge_count + 1, 3)


def project_mortar(incoming, amount, whole_k, is_stator, first_table, second_table):
    highest = lax.Precision.HIGHEST
    window = rotate_window(incoming, amount, whole_k, is_stator)
    edge_count = incoming.shape[-1]
    result = jnp.einsum(
        "mn,rnxe->rmxe", first_table, window[:, :, :, :edge_count], precision=highest
    )
    return result + jnp.einsum(
        "mn,rnxe->rmxe", second_table, window[:, :, :, 1:], precision=highest
    )


def local(field, coeffs, reaction, step_scale, rotation):
    side_index = lax.axis_index("side")
    lower = lax.axis_size("side") // 2 - 1
    cycle_length = field.shape[-1] * lax.axis_size("circ")
    is_stator = side_index > lower
    current = field[0]
    for step in range(STEPS):
        applied = element_apply(current, coeffs[0], reaction[0])
        zero_row = jnp.zeros_like(applied[:, 0, :, :1])
        summed = applied.at[:, 6].add(jnp.concatenate([applied[:, 0, :, 1:], zero_row], axis=2))
        summed = summed.at[:, 0].add(jnp.concatenate([zero_row, applied[:, 6, :, :-1]], axis=2))
        sector_rims = jnp.stack([applied[:, :, 0], applied[:, :, 6]])
        padded = padded_2(sector_rims, (("circ", 4),), 1, True)
        summed = summed.at[:, :, 6].add(padded[0, :, :, :, 2:])
        summed = summed.at[:, :, 0].add(padded[1, :, :, :, :-2])
        axial_faces = jnp.stack([applied[0], applied[6]])
        layered = padded_2(axial_faces, (("side", 0),), 1, False)
        below_top = layered[0]
        above_bottom = layered[3]
        offset = rotation[step]
        whole_k = offset // SUBSTEPS
        fraction = (offset % SUBSTEPS).astype(jnp.float32) / SUBSTEPS
        from_left, from_right = mortar_tables(fraction)
        first_table = jnp.where(is_stator, from_left, from_right.T)
        second_table = jnp.where(is_stator, from_right, from_left.T)
        amount = jnp.where(is_stator, whole_k, cycle_length - whole_k - 1)
        incoming = jnp.where(is_stator, below_top, above_bottom)
        contribution = project_mortar(
            incoming, amount, whole_k, is_stator, first_table, second_table
        )
        bottom_add = jnp.where(side_index == lower + 1, contribution, below_top)
        top_add = jnp.where(side_index == lower, contribution, above_bottom)
        summed = summed.at[0].add(bottom_add)
        summed = summed.at[6].add(top_add)
        current = current - step_scale[0] * summed
    return current[None]


N = 7
MESH = pl.DeviceIdType.MESH
CHUNKS = ((0, 3), (3, 4))
RIMS = (0, 6)
INNER = (1, 2, 3, 4, 5)
ONE_FIRST = (3, 2, 1, 0)
ONE_LAST = (7, 6, 5, 4)
FAR_FIRST = (5, 4, 7, 6, 3, 2, 1, 0)


def half_tables(matrix):
    minus = 0.5 * (matrix[:3, :3] - matrix[:3, :3:-1])
    plus = 0.5 * (matrix[:3, :3] + matrix[:3, :3:-1])
    return minus, plus


def weighted(constants, values):
    total = float(constants[0]) * values[0]
    for constant, value in zip(constants[1:], values[1:]):
        total = total + float(constant) * value
    return total


def derivative_of(u):
    table = derivative_table()
    minus, plus = half_tables(table)
    odd = [u[j] - u[6 - j] for j in range(3)]
    twice = u[3] + u[3]
    even = [(u[j] + u[6 - j]) - twice for j in range(3)]
    p = [weighted(minus[i], odd) for i in range(3)]
    q = [weighted(plus[i], even) for i in range(3)]
    middle = weighted(table[3, :3], odd)
    return [p[i] + q[i] for i in range(3)] + [middle] + [p[i] - q[i] for i in (2, 1, 0)]


def transposed_of(w):
    table = derivative_table().T
    minus, plus = half_tables(table)
    odd = [w[j] - w[6 - j] for j in range(3)]
    even = [w[j] + w[6 - j] for j in range(3)] + [w[3]]
    p = [weighted(minus[i], odd) for i in range(3)]
    q = [weighted(list(plus[i]) + [table[i, 3]], even) for i in range(3)]
    middle = -2.0 * (p[0] + p[1] + p[2])
    return [p[i] + q[i] for i in range(3)] + [middle] + [p[i] - q[i] for i in (2, 1, 0)]


def mortar_constants():
    points = gll_points()
    heights = (1.0 + points) * 0.5
    tables = np.zeros((SUBSTEPS, N, N), np.float32)
    on_left = np.zeros((SUBSTEPS, N), np.int32)
    for f in range(SUBSTEPS):
        fraction = f / SUBSTEPS
        for m in range(N):
            left = heights[m] < fraction
            on_left[f, m] = left
            place = 2.0 * (heights[m] - fraction + left) - 1.0
            for n in range(N):
                others = [q for q in range(N) if q != n]
                tables[f, m, n] = np.prod(
                    [(place - points[q]) / (points[n] - points[q]) for q in others]
                )
    return tables.reshape(-1), on_left.reshape(-1)


def rotated(value, shift, lane, sectors):
    width = value.shape[1]
    within = lax.rem(shift, width)
    whole = lax.rem(lax.div(shift, width), sectors)
    turned = pltpu.roll(value, within, 1)
    near = pltpu.roll(turned, whole, 0)
    far = pltpu.roll(near, 1, 0)
    return jnp.where(lane >= within, near, far)


def paired(index, mask, count):
    result, bit = 0, 1
    while bit < count:
        flip = (mask // bit) % 2
        result = result + bit * lax.rem(lax.div(index, bit) + flip, 2)
        bit *= 2
    return result


def step_kernel(
    lower, circ_count, first, workers, work_sides, rot_ref, table_ref, left_ref, field_ref,
    coeffs_ref, reaction_ref, scale_ref, out_ref, K, R, S, A, G, O, M, C, B, ends, ends_in,
    load_sem, conf_send, conf_recv, end_send, end_recv, one_send, one_recv, two_send, two_recv,
):
    U = out_ref.at[0]
    circ = lax.axis_index("circ")
    side = lax.axis_index("side")
    odd = lax.rem(side, 2)
    conf_a = 6 - 6 * odd
    mort_a = 6 * odd
    mate = side + 1 - 2 * odd
    at_interface = jnp.logical_or(side == lower, side == lower + 1)
    own_way = jnp.where(side == lower, 0, 1)
    central = jnp.logical_and(circ >= first, circ < first + workers)
    is_worker, side_place = [], []
    for sides in work_sides:
        is_here = side == sides[0]
        place = 0
        for i in range(1, len(sides)):
            is_here = jnp.logical_or(is_here, side == sides[i])
            place = place + jnp.where(side == sides[i], i, 0)
        is_worker.append(jnp.logical_and(central, is_here))
        side_place.append(place)
    slots = G.shape[1]
    locals_count = G.shape[2]
    near = 2 * lax.div(circ, circ_count // 2) + lax.rem(circ, 2)
    ahead = lax.rem(circ + 1, circ_count)
    behind = lax.rem(circ + circ_count - 1, circ_count)
    width = U.shape[-1]
    rows = U.shape[-2]
    lane = lax.broadcasted_iota(jnp.int32, (rows, width), 1)
    row = lax.broadcasted_iota(jnp.int32, (rows, width), 0)

    others = pl.ds(1 - odd, N - 1)
    face_loads = [
        pltpu.make_async_copy(field_ref.at[0], U, load_sem.at[0]),
        pltpu.make_async_copy(coeffs_ref.at[0, 0], K.at[0], load_sem.at[1]),
        pltpu.make_async_copy(reaction_ref.at[0, mort_a], R.at[mort_a], load_sem.at[2]),
        pltpu.make_async_copy(coeffs_ref.at[0, 1, mort_a], K.at[1, mort_a], load_sem.at[3]),
        pltpu.make_async_copy(coeffs_ref.at[0, 2, mort_a], K.at[2, mort_a], load_sem.at[4]),
    ]
    later_loads = [
        pltpu.make_async_copy(reaction_ref.at[0, others], R.at[others], load_sem.at[5]),
        pltpu.make_async_copy(coeffs_ref.at[0, 1, others], K.at[1, others], load_sem.at[6]),
        pltpu.make_async_copy(coeffs_ref.at[0, 2, others], K.at[2, others], load_sem.at[7]),
        pltpu.make_async_copy(scale_ref.at[0], S, load_sem.at[8]),
    ]
    for load in face_loads + later_loads:
        load.start()

    barrier = pltpu.get_barrier_semaphore()
    pl.semaphore_signal(
        barrier, inc=1, device_id={"circ": circ, "side": mate}, device_id_type=MESH
    )

    def greet(other_circ, other_side):
        pl.semaphore_signal(
            barrier, inc=1, device_id={"circ": other_circ, "side": other_side},
            device_id_type=MESH,
        )

    def greet_other(other_circ, other_side):
        @pl.when(jnp.logical_not(jnp.logical_and(circ == other_circ, side == other_side)))
        def _():
            greet(other_circ, other_side)

    every_side = sorted(set(work_sides[0] + work_sides[1]))
    works = jnp.logical_or(is_worker[0], is_worker[1])
    meets_self = jnp.logical_and(at_interface, works).astype(jnp.int32)

    @pl.when(at_interface)
    def _():
        for work_side in every_side:
            for w in range(first, first + workers):
                greet_other(w, work_side)

    @pl.when(works)
    def _():
        for c in range(circ_count):
            for face_side in (lower, lower + 1):
                greet_other(c, face_side)

    for other in (ahead, behind):
        greet(other, side)
    greeted = 3 + jnp.where(at_interface, workers * len(every_side), 0)
    greeted = greeted + jnp.where(works, 2 * circ_count, 0) - 2 * meets_self

    def barrier_wait():
        pl.semaphore_wait(barrier, greeted)

    derivative = derivative_table()
    is_odd = odd == 1
    column = [
        jnp.where(is_odd, float(derivative[p, 6]), float(derivative[p, 0])) for p in range(N)
    ]
    square = [
        jnp.where(is_odd, float(derivative[p, 6] ** 2), float(derivative[p, 0] ** 2))
        for p in range(N)
    ]
    planes = [jnp.where(is_odd, 0, N)] + list(range(1, N - 1)) + [jnp.where(is_odd, N, 6)]

    def line(direction, i, j, start=None):
        def at(p):
            return ((p, i, j), (i, p, j), (i, j, p))[direction]

        def to(p):
            return (planes[p], i, j) if direction == 0 else at(p)

        u = [U[at(p)] for p in range(N)]
        g = derivative_of(u)
        w = [g[p] * K[(direction,) + at(p)] for p in range(N)]
        y = transposed_of(w)
        for p in range(N):
            base = A[to(p)] if start is None else start(at(p), u[p])
            A[to(p)] = base + y[p]

    def reacted(at, u):
        return R[at] * u

    def mortar_start(at, u):
        _, r, c = at
        return B[0, r, c] + B[1, r, c] * u

    def circ_lines(plane):
        for r in range(N):
            line(2, plane, r)

    def radial_lines(plane, columns):
        for c in columns:
            line(1, plane, c, reacted)

    def partial_axial(columns):
        @pl.loop(0, N)
        def _(r):
            for c in columns:
                u = [U[p, r, c] for p in range(N)]
                u[0] = jnp.where(is_odd, u[0], 0.0)
                u[6] = jnp.where(is_odd, 0.0, u[6])
                g = derivative_of(u)
                total = column[0] * (g[0] * K[0, 0, r, c])
                for p in range(1, N):
                    total = total + column[p] * (g[p] * K[0, p, r, c])
                B[0, r, c] = total

    def first_lines():
        for load in later_loads:
            load.wait()

        @pl.loop(0, N - 1)
        def _(q):
            radial_lines(q + 1 - odd, INNER)

    for load in face_loads:
        load.wait()
    partial_axial(range(N))

    @pl.loop(0, N)
    def _(r):
        for c in range(N):
            total = R[mort_a, r, c]
            for p in range(N):
                total = total + square[p] * K[0, p, r, c]
            B[1, r, c] = total

    barrier_wait()

    def update_plane(a, columns, from_ahead, from_behind, extra):
        for r in range(N):
            i = a * N + r
            for c in columns:
                s = A[a, r, c]
                if r == 6:
                    s = s + jnp.where(row < rows - 1, pltpu.roll(A[a, 0, c], rows - 1, 0), 0.0)
                if r == 0:
                    s = s + jnp.where(row > 0, pltpu.roll(A[a, 6, c], 1, 0), 0.0)
                if c == 6:
                    s = s + jnp.where(
                        lane == width - 1,
                        pltpu.roll(from_ahead, width - 1 - i, 1),
                        pltpu.roll(A[a, r, 0], width - 1, 1),
                    )
                if c == 0:
                    s = s + jnp.where(
                        lane == 0,
                        pltpu.roll(from_behind, lax.rem(width - i, width), 1),
                        pltpu.roll(A[a, r, 6], 1, 1),
                    )
                if extra is not None:
                    s = s + extra[r, c]
                U[a, r, c] = U[a, r, c] - S[a, r, c] * s

    def one_step(t, _):
        par = lax.rem(t, 2)

        def conf_copy():
            return pltpu.make_async_remote_copy(
                src_ref=A.at[conf_a], dst_ref=C.at[par], send_sem=conf_send,
                recv_sem=conf_recv.at[par], device_id={"circ": circ, "side": mate},
                device_id_type=MESH,
            )

        def end_copy(which, target):
            return pltpu.make_async_remote_copy(
                src_ref=ends.at[which], dst_ref=ends_in.at[par, which],
                send_sem=end_send.at[which], recv_sem=end_recv.at[par, which],
                device_id={"circ": target, "side": side}, device_id_type=MESH,
            )

        def remote(src, dst, send_sem, recv_sem, to_circ, to_side):
            return pltpu.make_async_remote_copy(
                src_ref=src, dst_ref=dst, send_sem=send_sem, recv_sem=recv_sem,
                device_id={"circ": to_circ, "side": to_side}, device_id_type=MESH,
            )

        def start(src, dst, send_sem, recv_sem, to_circ, to_side, can_be_here):
            copy = remote(src, dst, send_sem, recv_sem, to_circ, to_side)
            if not can_be_here:
                copy.start()
                return
            here = jnp.logical_and(to_circ == circ, to_side == side)

            @pl.when(jnp.logical_not(here))
            def _():
                copy.start()

            @pl.when(here)
            def _():
                pltpu.make_async_copy(src, dst, recv_sem).start()

        def wait_sent(sent, send_sem, one_here):
            def wait(ref):
                remote(ref, ref, send_sem, send_sem, circ, mate).wait_send()

            @pl.when(one_here)
            def _():
                wait(sent.at[..., pl.ds(0, rows - 1), :])

            @pl.when(jnp.logical_not(one_here))
            def _():
                wait(sent)

        def arrived(ref, recv_sem):
            remote(ref, ref, recv_sem, recv_sem, circ, mate).wait_recv()

        own_slot = own_way if slots > 1 else 0

        def start_one(h, d):
            rows_of = pl.ds(*CHUNKS[h])
            place = paired(near, d % workers, workers)
            turn = d // workers
            count = len(work_sides[0])
            near_at = own_way if count > 1 else 0
            at = lax.rem(near_at + turn, count)
            to_side = jnp.where(side == lower, work_sides[0][0], work_sides[1][0])
            for i in range(1, count):
                other = jnp.where(side == lower, work_sides[0][i], work_sides[1][i])
                to_side = jnp.where(at == i, other, to_side)
            group = turn // count
            start(
                A.at[mort_a, rows_of, :, pl.ds((group * count + at) * workers + place, 1), :],
                G.at[par, own_slot, group, rows_of, :, pl.ds(circ, 1), :],
                one_send, one_recv.at[par, h, own_slot], first + place, to_side,
                d % workers == 0 and turn % count == 0,
            )

        def start_two(way, h, j, d):
            rows_of = pl.ds(*CHUNKS[h])
            target = paired(circ, d, circ_count)
            slot = way if slots > 1 else 0
            place = (j * len(work_sides[way]) + side_place[way]) * workers + circ - first
            start(
                O.at[slot, j, rows_of, :, pl.ds(target, 1), :],
                M.at[par, rows_of, :, pl.ds(place, 1), :],
                two_send.at[slot], two_recv.at[par, h], target, lower + 1 - way,
                d == 0 and lower + 1 - way in work_sides[way],
            )

        for q in range(N):
            line(1, mort_a, q, mortar_start)
        for h, (begin, count) in enumerate(CHUNKS):
            for q in range(begin, begin + count):
                line(2, mort_a, q)

            @pl.when(at_interface)
            def _():
                for d in ONE_FIRST:
                    start_one(h, d)
                if h == len(CHUNKS) - 1:
                    for g in range(len(CHUNKS)):
                        for d in ONE_LAST:
                            start_one(g, d)

        @pl.when(t == 0)
        def _():
            first_lines()

        @pl.loop(0, N - 1)
        def _(q):
            radial_lines(q + 1 - odd, RIMS)
            circ_lines(q + 1 - odd)

        def axial_lines(columns):
            @pl.loop(0, N)
            def _(r):
                for c in columns:
                    line(0, r, c)

        axial_lines(RIMS)
        low = jnp.zeros((rows, width), jnp.float32)
        high = low
        for i in range(N * N):
            low = jnp.where(lane == i, pltpu.roll(A[i // N, i % N, 0], i, 1), low)
            high = jnp.where(lane == i, pltpu.roll(A[i // N, i % N, 6], i + 1, 1), high)
        ends[0] = low
        ends[1] = high
        end_copy(0, behind).start()
        end_copy(1, ahead).start()
        axial_lines(INNER)
        conf_copy().start()

        def inner_plane(a, extra):
            update_plane(a, INNER, None, None, extra)

            @pl.when(t < STEPS - 1)
            def _():
                radial_lines(a, INNER)

        @pl.loop(1, N - 1)
        def _(a):
            inner_plane(a, None)

        offset = rot_ref[t]
        k = lax.div(offset, SUBSTEPS)
        f = offset - SUBSTEPS * k
        cycle = circ_count * width

        def stator_rows(slot, places):
            values = [[G[par, slot, j, r, n] for n in range(N)] for j, r in places]
            for m in range(N):
                factors = [table_ref[f * N * N + m * N + n] for n in range(N)]
                shift = k + left_ref[f * N + m]
                for (j, r), own in zip(places, values):
                    total = factors[0] * own[0]
                    for n in range(1, N):
                        total = total + factors[n] * own[n]
                    O[slot, j, r, m] = rotated(total, shift, lane, circ_count)

        def rotor_rows(slot, places):
            shifts = [cycle - k - left_ref[f * N + m] for m in range(N)]
            values = [
                [rotated(G[par, slot, j, r, m], shifts[m], lane, circ_count) for m in range(N)]
                for j, r in places
            ]
            for n in range(N):
                factors = [table_ref[f * N * N + m * N + n] for m in range(N)]
                for (j, r), own in zip(places, values):
                    total = factors[0] * own[0]
                    for m in range(1, N):
                        total = total + factors[m] * own[m]
                    O[slot, j, r, n] = total

        def serve(way, h):
            begin, count = CHUNKS[h]
            slot = way if slots > 1 else 0
            arrived(G.at[par, slot, :, pl.ds(begin, count)], one_recv.at[par, h, slot])
            for j in range(locals_count):
                project = (stator_rows, rotor_rows)[way]
                project(slot, [(j, r) for r in range(begin, begin + count)])
                for d in FAR_FIRST:
                    start_two(way, h, j, d)

        for work_side in sorted(set(work_sides[0] + work_sides[1])):
            near_way = 0 if work_side <= lower else 1

            @pl.when(jnp.logical_and(central, side == work_side))
            def _():
                for other, h in ((0, 0), (0, 1), (1, 0), (1, 1)):
                    way = (near_way + other) % 2
                    if work_side in work_sides[way]:
                        serve(way, h)

        conf_copy().wait_recv()
        conf_copy().wait_send()
        inner_plane(conf_a, C.at[par])

        @pl.when(t < STEPS - 1)
        def _():
            partial_axial(INNER)

        end_copy(0, behind).wait_recv()
        end_copy(1, ahead).wait_recv()
        from_ahead = ends_in[par, 0]
        from_behind = ends_in[par, 1]

        def rim_plane(a, extra):
            update_plane(a, RIMS, from_ahead, from_behind, extra)

        @pl.loop(1, N - 1)
        def _(a):
            rim_plane(a, None)

        rim_plane(conf_a, C.at[par])

        @pl.when(t < STEPS - 1)
        def _():
            partial_axial(RIMS)

        @pl.when(at_interface)
        def _():
            for h in range(len(CHUNKS)):
                arrived(M.at[par, pl.ds(*CHUNKS[h])], two_recv.at[par, h])
            update_plane(mort_a, range(N), from_ahead, from_behind, M.at[par])
            to_self = False
            for way in range(2):
                if lower + way in work_sides[way]:
                    to_self = jnp.logical_or(
                        to_self, jnp.logical_and(is_worker[way], own_way == way)
                    )
            wait_sent(A.at[mort_a], one_send, jnp.asarray(to_self))

        for way in range(2):
            @pl.when(is_worker[way])
            def _():
                slot = way if slots > 1 else 0
                wait_sent(O.at[slot], two_send.at[slot], side == lower + 1 - way)

        @pl.when(jnp.logical_not(at_interface))
        def _():
            update_plane(mort_a, range(N), from_ahead, from_behind, None)

        end_copy(0, behind).wait_send()
        end_copy(1, ahead).wait_send()
        return 0

    lax.fori_loop(0, STEPS, one_step, 0)


def placed_work(circ_count, lower):
    return circ_count // 4, circ_count // 2, ((lower, lower + 2), (lower, lower + 2))


def fused(mesh, field, coeffs, reaction, step_scale, rotation):
    circ_count = mesh.shape["circ"]
    lower = mesh.shape["side"] // 2 - 1
    first, workers, work_sides = placed_work(circ_count, lower)
    kinds = len(set(work_sides[0]) & set(work_sides[1])) > 0
    slots = 2 if kinds else 1
    rows_each = circ_count // (workers * len(work_sides[0]))
    node_shape = field.shape[1:]
    face_shape = node_shape[1:]
    tile = face_shape[2:]
    tables, on_left = mortar_constants()
    smem = pl.BlockSpec(memory_space=pltpu.SMEM)
    anywhere = pl.BlockSpec(memory_space=pl.ANY)
    dma = pltpu.SemaphoreType.DMA
    f32 = jnp.float32
    operands = (
        rotation, jnp.asarray(tables), jnp.asarray(on_left), field, coeffs, reaction, step_scale
    )
    return pl.pallas_call(
        partial(step_kernel, lower, circ_count, first, workers, work_sides),
        out_shape=jax.ShapeDtypeStruct(field.shape, f32),
        in_specs=[smem, smem, smem] + [anywhere] * 4,
        out_specs=pl.BlockSpec(memory_space=pltpu.VMEM),
        scratch_shapes=[
            pltpu.VMEM(coeffs.shape[1:], f32),
            pltpu.VMEM(node_shape, f32),
            pltpu.VMEM(node_shape, f32),
            pltpu.VMEM((N + 1,) + face_shape, f32),
            pltpu.VMEM((2, slots, rows_each) + face_shape, f32),
            pltpu.VMEM((slots, rows_each) + face_shape, f32),
            pltpu.VMEM((2,) + face_shape, f32),
            pltpu.VMEM((2,) + face_shape, f32),
            pltpu.VMEM((2,) + face_shape, f32),
            pltpu.VMEM((2,) + tile, f32),
            pltpu.VMEM((2, 2) + tile, f32),
            dma((9,)),
            dma(()),
            dma((2,)),
            dma((2,)),
            dma((2, 2)),
            dma(()),
            dma((2, len(CHUNKS), slots)),
            dma((slots,)),
            dma((2, len(CHUNKS))),
        ],
        compiler_params=pltpu.CompilerParams(
            collective_id=0, has_side_effects=True, vmem_limit_bytes=24 * 2**20
        ),
    )(*[pltpu.with_memory_space_constraint(operand, pltpu.HBM) for operand in operands])


def solution(mesh):
    def body(field, coeffs, reaction, step_scale, rotation):
        radial_count, lanes = field.shape[-2:]
        whole_circle = radial_count == mesh.shape["circ"] == 8 and lanes == 128
        if whole_circle and mesh.shape["side"] == 4:
            return fused(mesh, field, coeffs, reaction, step_scale, rotation)
        return local(field, coeffs, reaction, step_scale, rotation)

    in_specs = (
        P("side", None, None, None, None, "circ"),
        P("side", None, None, None, None, None, "circ"),
        P("side", None, None, None, None, "circ"),
        P("side", None, None, None, None, "circ"),
        P(),
    )
    out_specs = P("side", None, None, None, None, "circ")
    return jax.shard_map(body, mesh=mesh, in_specs=in_specs, out_specs=out_specs, check_vma=False)
```
